32 devices in a mesh: section: 8 (over z, y), tensor: 4 (over x, core).
Axes of the slice: x: 2, y: 2, z: 4, core: 2. Of those that a mesh axis runs over, the one named last changes fastest.
Arguments:
- inputs: bfloat16 [2, 163840], P(None, 'tensor'), may hold values from -6 to 6
- cotangent: bfloat16 [2, 163840], P(None, 'tensor'), may hold values from -6 to 6
- weights: bfloat16 [8, 2560, 10240], P('section', None, 'tensor'), may hold values from -0.0625 to 0.0625
- norm_gains: float32 [4, 2560], replicated, may hold values from 0.5 to 1.5
Outputs:
- layer_results: bfloat16 [8, 2, 163840], P('section', None, 'tensor')
The draws below stay inside these ranges and needn't reach their ends.
All inputs are finite; a program needn't handle non-finite values.
Results may differ from the reference program's by a relative error of at most 0.02.
Values may be sent and summed in bfloat16 or wider, within the bound.
No kernel may reach another device: no remote copies, remote signals or barrier semaphores. Data moves between devices by JAX's collectives and lax.ppermute only.
A program may use at most 64 MiB of HBM per device.

```python
import jax
import jax.numpy as jnp
from jax import lax

D = 2560
FF = 10240
LAYERS = 4
R = 64
M = 2
MB_TOTAL = 2
ALL_LAYERS = 4
N_SECTION = 8
N_TENSOR = 4


def level_of(stream_key, extent, split, least, high):
    gain = 1.0
    for axis_at, blocks in split:
        heights = jax.random.uniform(jax.random.fold_in(jax.random.fold_in(stream_key, 6), axis_at), (blocks,), jnp.float32, least / len(split), high / len(split))
        gain = gain * jnp.repeat(jnp.exp(heights), extent[axis_at] // blocks).reshape((-1,) + (1,) * (len(extent) - 1 - axis_at))
    return gain


def centred(stream_key, shape, width, bound, shards=(), kind=jnp.bfloat16):
    entries = width * jax.random.normal(stream_key, shape, jnp.float32)
    if shards:
        entries = entries * level_of(stream_key, shape, shards, -0.22, 0.18)
    return jnp.clip(entries, -bound, bound).astype(kind)


def setup_inputs(seed: int = 0) -> dict:
    streams_of = jax.random.split(jax.random.key(seed), 5)
    return {
        "inputs": centred(streams_of[0], (MB_TOTAL, R * D), 1.0, 6.0, ((1, 4),)),
        "cotangent": centred(streams_of[1], (MB_TOTAL, R * D), 1.0, 6.0, ((1, 4),)),
        "weights": centred(streams_of[2], (N_SECTION, D, FF), FF ** -0.5, 0.0625, ((0, 8), (2, 4))),
        "norm_gains": jnp.clip(1.0 + 0.1 * jax.random.normal(streams_of[3], (ALL_LAYERS, D), jnp.float32), 0.5, 1.5),
    }


epsilon = 1e-05

def gelu_tanh(values):
    return jax.nn.gelu(values, approximate=True)

def normalize(carried):
    widened = carried.astype(jnp.float32)
    inverse_rms = lax.rsqrt(lax.optimization_barrier(jnp.mean(widened * widened, axis=-1, keepdims=True)) + epsilon)
    return (widened * inverse_rms, inverse_rms)

def block_sum(operand, weight):
    row_total = operand.shape[0]
    feature_count = weight.shape[0]
    block_width = FF // N_TENSOR
    operand_blocks = operand.reshape(row_total, N_TENSOR, block_width).astype(jnp.float32)
    weight_blocks = weight.reshape(feature_count, N_TENSOR, block_width).astype(jnp.float32)
    partials = jnp.einsum('rjb,djb->jrd', operand_blocks, weight_blocks)
    rounded = lax.optimization_barrier(partials.astype(jnp.bfloat16))
    return lax.optimization_barrier(jnp.sum(rounded.astype(jnp.float32), axis=0))

def run_stack(stack_index, stack_count, inputs, cotangent, weights, norm_gains):
    stride = 2 * stack_count
    carried = inputs[stack_index * M:(stack_index + 1) * M].reshape(M * R, D)
    saved_inputs = []
    layer_outputs = []
    for layer_index in range(LAYERS):
        up_weight = weights[layer_index * stride + 2 * stack_index]
        down_weight = weights[layer_index * stride + 2 * stack_index + 1]
        gain_row = norm_gains[stack_index * LAYERS + layer_index]
        unit_rows, _ = normalize(carried)
        normed = (unit_rows * gain_row).astype(jnp.bfloat16)
        preact = jnp.dot(normed, up_weight, preferred_element_type=jnp.float32)
        hidden = gelu_tanh(preact).astype(jnp.bfloat16)
        branch = block_sum(hidden, down_weight)
        saved_inputs.append(carried)
        carried = (carried.astype(jnp.float32) + branch).astype(jnp.bfloat16)
        layer_outputs.append(carried)
    gradient = cotangent[stack_index * M:(stack_index + 1) * M].reshape(M * R, D)
    layer_grads = [None] * LAYERS
    for layer_index in reversed(range(LAYERS)):
        up_weight = weights[layer_index * stride + 2 * stack_index]
        down_weight = weights[layer_index * stride + 2 * stack_index + 1]
        gain_row = norm_gains[stack_index * LAYERS + layer_index]
        grad_hidden = jnp.dot(gradient, down_weight, preferred_element_type=jnp.float32).astype(jnp.bfloat16)
        unit_rows, inverse_rms = normalize(saved_inputs[layer_index])
        normed = (unit_rows * gain_row).astype(jnp.bfloat16)
        preact = jnp.dot(normed, up_weight, preferred_element_type=jnp.float32)
        _, pullback = jax.vjp(gelu_tanh, preact)
        grad_pre = pullback(grad_hidden.astype(jnp.float32))[0].astype(jnp.bfloat16)
        grad_normed = block_sum(grad_pre, up_weight)
        grad_unit = grad_normed * gain_row
        grad_input = inverse_rms * (grad_unit - unit_rows * lax.optimization_barrier(jnp.mean(grad_unit * unit_rows, axis=-1, keepdims=True)))
        gradient = (gradient.astype(jnp.float32) + grad_input).astype(jnp.bfloat16)
        layer_grads[layer_index] = gradient
    return (layer_grads, layer_outputs)

def reference(inputs, cotangent, weights, norm_gains):
    stack_count = N_SECTION // (2 * LAYERS)
    stride = 2 * stack_count
    everything = [None] * N_SECTION
    for stack_index in range(stack_count):
        grads, outputs = run_stack(stack_index, stack_count, inputs, cotangent, weights, norm_gains)
        for layer_index in range(LAYERS):
            position = layer_index * stride + 2 * stack_index
            everything[position] = grads[layer_index].reshape(M, R * D)
            everything[position + 1] = outputs[layer_index].reshape(M, R * D)
    return jnp.stack(everything)
```

```python
import jax
import jax.numpy as jnp
from jax import lax
from jax.sharding import PartitionSpec as P

LAYERS = 4
epsilon = 1e-05
AXES = ("section", "tensor")


def gelu_both(v):
    c = 0.7978845608028654
    v2 = v * v
    th = jnp.tanh(c * v * (1.0 + 0.044715 * v2))
    half = 0.5 * (1.0 + th)
    value = v * half
    slope = half + 0.5 * v * (1.0 - th * th) * (c * (1.0 + 3 * 0.044715 * v2))
    return value, slope


def inverse_rms_of(rows):
    return lax.rsqrt(jnp.mean(rows * rows, axis=-1, keepdims=True) + epsilon)


def body(inputs, cotangent, weights, norm_gains):
    S = lax.axis_size("section")
    T = lax.axis_size("tensor")
    stacks = S // (2 * LAYERS)
    stride = 2 * stacks
    si = lax.axis_index("section")
    ti = lax.axis_index("tensor")
    core = ti % 2
    group = si % stride // 2
    layer = si // stride
    up = si % 2 == 0
    w = weights[0]
    D = w.shape[0]
    B = inputs.shape[0] // stacks
    share = inputs.shape[1] // D
    hi = T // 2
    half_rows = hi * share
    rows = T * share
    steps = B + 2 * (LAYERS - 1)
    top = 2 * (LAYERS - 1)
    f32, bf16 = jnp.float32, jnp.bfloat16

    def send(x, pairs, flip=0):
        route = [(a * T + t, b * T + (t ^ flip)) for a, b in pairs for t in range(T)]
        return lax.ppermute(x, AXES, route)

    every = [(s, s) for s in range(S)]

    def section(k, q, down):
        return k * stride + 2 * q + down

    def live(t):
        fwd = [k for k in range(LAYERS) if 0 <= t - k < B]
        bwd = [k for k in range(LAYERS) if 0 <= t - top + k < B]
        return fwd, bwd

    gain = lax.dynamic_index_in_dim(norm_gains, group * LAYERS + layer, 0, keepdims=True)
    own_in = lax.dynamic_slice_in_dim(inputs, group * B, B, 0).reshape(B, share, D)
    own_cot = lax.dynamic_slice_in_dim(cotangent, group * B, B, 0).reshape(B, share, D)

    def spread(x):
        x = x[None]
        for bit in range(1, T.bit_length() - 1):
            got = send(x, every, 1 << bit)
            mine_high = (ti >> bit) % 2 == 1
            x = jnp.where(
                mine_high,
                jnp.concatenate([got, x], 0),
                jnp.concatenate([x, got], 0),
            )
        return x

    def join_cores(part):
        got = send(part, every, 1)
        return jnp.where(
            core == 1, jnp.stack([got, part], 1), jnp.stack([part, got], 1)
        ).reshape(rows, D)

    main_seed = [spread(jnp.where(up, own_in[b], own_cot[b])) for b in range(B)]
    rest_seed = [spread(jnp.where(up, own_cot[b], own_in[b])) for b in range(B)]

    main = main_seed[0]
    rest = rest_seed[0]
    slope_stash = jnp.zeros((B, rows, w.shape[1]), bf16)
    part_stash = jnp.zeros((B, hi, share, D), bf16)
    results = jnp.zeros((B, share, D), bf16)
    edge_up = up & (layer == 0)
    edge_down = (~up) & (layer == LAYERS - 1)

    for t in range(steps):
        fwd, bwd = live(t)
        fb = jnp.clip(t - layer, 0, B - 1)
        bb = jnp.clip(t - top + layer, 0, B - 1)
        f_ok = (t - layer >= 0) & (t - layer < B)
        b_ok = (t - top + layer >= 0) & (t - top + layer < B)
        if t < B:
            main = jnp.where(edge_up, main_seed[t], main)
            rest = jnp.where((~up) & (layer == 0), rest_seed[t], rest)
        tb = t - (LAYERS - 1)
        if 0 <= tb < B:
            main = jnp.where(edge_down, main_seed[tb], main)
            rest = jnp.where(up & (layer == LAYERS - 1), rest_seed[tb], rest)
        full = join_cores(main)
        old = lax.dynamic_index_in_dim(part_stash, fb, 0, keepdims=False)
        part_stash = lax.dynamic_update_index_in_dim(
            part_stash, jnp.where(f_ok, main, old), fb, 0
        )
        wide = full.astype(f32)
        normed = wide * inverse_rms_of(wide) * gain
        operand = jnp.where(up, normed, wide).astype(bf16)
        y = jnp.dot(operand, w, preferred_element_type=f32)
        value, slope = gelu_both(y)
        outgoing = jnp.where(up, value, y).astype(bf16)
        old = lax.dynamic_index_in_dim(slope_stash, fb, 0, keepdims=False)
        slope_stash = lax.dynamic_update_index_in_dim(
            slope_stash, jnp.where(f_ok, slope.astype(bf16), old), fb, 0
        )
        pairs = [(section(k, q, 0), section(k, q, 1)) for k in fwd for q in range(stacks)]
        pairs += [(section(k, q, 1), section(k, q, 0)) for k in bwd for q in range(stacks)]
        arrived = send(outgoing, pairs)
        slope = lax.dynamic_index_in_dim(slope_stash, bb, 0, keepdims=False)
        operand = jnp.where(
            up, (arrived.astype(f32) * slope.astype(f32)).astype(bf16), arrived
        )
        partial = lax.dot_general(
            operand, w, (((1,), (1,)), ((), ())), preferred_element_type=f32
        ).reshape(hi, 2, share, D)
        keep = jnp.where(core == 1, partial[:, 1], partial[:, 0])
        give = jnp.where(core == 1, partial[:, 0], partial[:, 1]).astype(bf16)
        active = [section(k, q, 1) for k in fwd for q in range(stacks)]
        active += [section(k, q, 0) for k in bwd for q in range(stacks)]
        here = [(s, s) for s in active]
        total = keep + send(give, here, 1).astype(f32)
        for bit in range(1, T.bit_length() - 1):
            mine = total.astype(bf16)
            total = mine.astype(f32) + send(mine, here, 1 << bit).astype(f32)
        saved = lax.dynamic_index_in_dim(part_stash, bb, 0, keepdims=False).astype(f32)
        scale = inverse_rms_of(saved)
        unit = saved * scale
        grad_unit = total * gain
        grad_in = scale * (grad_unit - unit * jnp.mean(grad_unit * unit, axis=-1, keepdims=True))
        new = (rest.astype(f32) + jnp.where(up, grad_in, total)).astype(bf16)
        mine = lax.dynamic_index_in_dim(new, ti // 2, 0, keepdims=False)
        slot = jnp.where(up, bb, fb)
        ok = jnp.where(up, b_ok, f_ok)
        old = lax.dynamic_index_in_dim(results, slot, 0, keepdims=False)
        results = lax.dynamic_update_index_in_dim(results, jnp.where(ok, mine, old), slot, 0)
        if t + 1 < steps:
            cross = [
                (section(k, q, 1), section(k + 1, q, 0))
                for k in fwd if k + 1 < LAYERS for q in range(stacks)
            ] + [
                (section(k, q, 0), section(k - 1, q, 1))
                for k in bwd if k > 0 for q in range(stacks)
            ]
            along = [
                (section(k, q, 1), section(k + 1, q, 1))
                for k in fwd if k + 1 < LAYERS for q in range(stacks)
            ] + [
                (section(k, q, 0), section(k - 1, q, 0))
                for k in bwd if k > 0 for q in range(stacks)
            ]
            main = send(new, cross)
            rest = send(new, along)
    return results.reshape(1, B, share * D)


def solution(mesh):
    placed = (P(None, "tensor"), P(None, "tensor"), P("section", None, "tensor"), P())
    return jax.shard_map(
        body, mesh=mesh, in_specs=placed, out_specs=P("section", None, "tensor"), check_vma=False
    )
```

```python
import functools

import jax
import jax.numpy as jnp
from jax import lax
from jax.experimental import pallas as pl
from jax.experimental.pallas import tpu as pltpu
from jax.sharding import PartitionSpec as P

LAYERS = 4
epsilon = 1e-05
AXES = ("section", "tensor")
f32, bf16 = jnp.float32, jnp.bfloat16
VMEM = pl.BlockSpec(memory_space=pltpu.VMEM)
SMEM = pl.BlockSpec(memory_space=pltpu.SMEM)
HBM = pl.BlockSpec(memory_space=pl.ANY)


def params(mib=8):
    return pltpu.CompilerParams(vmem_limit_bytes=mib * 1024 * 1024)


def tile_of(width):
    for tile in (512, 256, 128):
        if width % tile == 0:
            return tile
    return width


def gelu_both(v):
    c = 0.7978845608028654
    v2 = v * v
    th = jnp.tanh(c * v * (1.0 + 0.044715 * v2))
    half = 0.5 * (1.0 + th)
    slope = half + 0.5 * v * (1.0 - th * th) * (c * (1.0 + 3 * 0.044715 * v2))
    return v * half, slope


def inverse_rms_of(rows):
    return lax.rsqrt(jnp.mean(rows * rows, axis=-1, keepdims=True) + epsilon)


def load_weights(w):
    def kernel(src, dst, sem):
        copy = pltpu.make_async_copy(src, dst, sem)
        copy.start()
        copy.wait()

    return pl.pallas_call(
        kernel,
        in_specs=[HBM],
        out_specs=VMEM,
        out_shape=pltpu.VMEM(w.shape, w.dtype),
        scratch_shapes=[pltpu.SemaphoreType.DMA(())],
        compiler_params=params(16),
        name="load_weights",
    )(w)


def first_kernel(mode, tile, *refs):
    if mode == "fwd":
        part, got, gain, w, out, slope, a = refs
        up = None
    elif mode == "bwd":
        part, got, w, out, a = refs
    else:
        flag, part, got, gain, w, out, slope, a = refs
        up = flag[0] == 1
    h = part.shape[0]
    for i, ref in enumerate((part, got)):
        if mode == "bwd":
            a[i * h:(i + 1) * h] = ref[...]
        else:
            x = ref[...].astype(f32)
            n = (x * inverse_rms_of(x) * gain[...]).astype(bf16)
            if up is not None:
                n = jnp.where(up, n, ref[...])
            a[i * h:(i + 1) * h] = n

    def step(i, carry):
        at = pl.ds(pl.multiple_of(i * tile, tile), tile)
        y = jnp.dot(a[...], w[:, at], preferred_element_type=f32)
        if mode == "bwd":
            out[:, at] = y.astype(bf16)
        else:
            value, grad = gelu_both(y)
            slope[:, at] = grad.astype(bf16)
            if up is not None:
                value = jnp.where(up, value, y)
            out[:, at] = value.astype(bf16)
        return carry

    lax.fori_loop(0, w.shape[1] // tile, step, 0)


def first(mode, flag, part, got, gain, w):
    rows = 2 * part.shape[0]
    D, F = w.shape
    shape = jax.ShapeDtypeStruct((rows, F), bf16)
    args = {"fwd": (part, got, gain, w), "bwd": (part, got, w)}.get(
        mode, (flag, part, got, gain, w)
    )
    specs = [VMEM] * len(args)
    if mode == "mix":
        specs[0] = SMEM
    count = 1 if mode == "bwd" else 2
    return pl.pallas_call(
        functools.partial(first_kernel, mode, tile_of(F)),
        in_specs=specs,
        out_specs=[VMEM] * count,
        out_shape=[shape] * count,
        scratch_shapes=[pltpu.VMEM((rows, D), bf16)],
        compiler_params=params(),
        cost_estimate=pl.CostEstimate(
            flops=2 * rows * D * F, bytes_accessed=2 * D * F, transcendentals=rows * F
        ),
        name="first_" + mode,
    )(*args)


def second_kernel(mode, tile, *refs):
    if mode == "fwd":
        arrived, w, keep, give, a = refs
        src = arrived
    elif mode == "bwd":
        arrived, slope, w, keep, give, a = refs
    else:
        flag, arrived, slope, w, keep, give, a = refs
    if mode == "fwd":
        a = arrived
    else:
        z = arrived[...]
        d = (z.astype(f32) * slope[...].astype(f32)).astype(bf16)
        if mode == "mix":
            d = jnp.where(flag[0] == 1, d, z)
        a[...] = d
    h = keep.shape[0]

    def step(i, carry):
        at = pl.ds(pl.multiple_of(i * tile, tile), tile)
        y = lax.dot_general(
            a[...], w[at, :], (((1,), (1,)), ((), ())), preferred_element_type=f32
        )
        keep[:, at] = y[:h]
        give[:, at] = y[h:].astype(bf16)
        return carry

    lax.fori_loop(0, w.shape[0] // tile, step, 0)


def second(mode, flag, arrived, slope, w):
    rows, F = arrived.shape
    D = w.shape[0]
    args = {"fwd": (arrived, w), "bwd": (arrived, slope, w)}.get(
        mode, (flag, arrived, slope, w)
    )
    specs = [VMEM] * len(args)
    if mode == "mix":
        specs[0] = SMEM
    return pl.pallas_call(
        functools.partial(second_kernel, mode, tile_of(D)),
        in_specs=specs,
        out_specs=[VMEM] * 2,
        out_shape=[
            jax.ShapeDtypeStruct((rows // 2, D), f32),
            jax.ShapeDtypeStruct((rows // 2, D), bf16),
        ],
        scratch_shapes=[pltpu.VMEM((rows, F), bf16)],
        compiler_params=params(),
        cost_estimate=pl.CostEstimate(
            flops=2 * rows * D * F, bytes_accessed=2 * D * F, transcendentals=0
        ),
        name="second_" + mode,
    )(*args)


def finish_kernel(mode, *refs):
    if mode == "fwd":
        total, got, rest, out = refs
        out[...] = (
            rest[...].astype(f32) + (total[...].astype(f32) + got[...].astype(f32))
        ).astype(bf16)
        return
    if mode == "bwd":
        total, got, rest, saved, gain, out = refs
    else:
        flag, total, got, rest, saved, gain, out = refs
    summed = total[...].astype(f32) + got[...].astype(f32)
    x = saved[...].astype(f32)
    scale = inverse_rms_of(x)
    unit = x * scale
    gu = summed * gain[...]
    delta = scale * (gu - unit * jnp.mean(gu * unit, axis=-1, keepdims=True))
    if mode == "mix":
        delta = jnp.where(flag[0] == 1, delta, summed)
    out[...] = (rest[...].astype(f32) + delta).astype(bf16)


def finish(mode, flag, total, got, rest, saved, gain):
    args = {
        "fwd": (total, got, rest),
        "bwd": (total, got, rest, saved, gain),
    }.get(mode, (flag, total, got, rest, saved, gain))
    specs = [VMEM] * len(args)
    if mode == "mix":
        specs[0] = SMEM
    return pl.pallas_call(
        functools.partial(finish_kernel, mode),
        in_specs=specs,
        out_specs=VMEM,
        out_shape=jax.ShapeDtypeStruct(rest.shape, bf16),
        compiler_params=params(),
        name="finish_" + mode,
    )(*args)


def body(inputs, cotangent, weights, norm_gains):
    S = lax.axis_size("section")
    T = lax.axis_size("tensor")
    stacks = S // (2 * LAYERS)
    stride = 2 * stacks
    si = lax.axis_index("section")
    ti = lax.axis_index("tensor")
    group = si % stride // 2
    layer = si // stride
    up = si % 2 == 0
    D = weights.shape[1]
    B = inputs.shape[0] // stacks
    share = inputs.shape[1] // D
    hi = T // 2
    h = hi * share
    top = 2 * (LAYERS - 1)
    bits = T.bit_length() - 1

    def send(x, pairs, flip=0):
        route = [(a * T + t, b * T + (t ^ flip)) for a, b in pairs for t in range(T)]
        return lax.ppermute(x, AXES, route)

    def section(k, q, down):
        return k * stride + 2 * q + down

    def each(pairs):
        return [(section(a, q, i), section(b, q, j)) for a, i, b, j in pairs for q in range(stacks)]

    gain = lax.dynamic_index_in_dim(norm_gains, group * LAYERS + layer, 0, keepdims=True)
    flag = jnp.where(up, 1, 0).astype(jnp.int32).reshape(1)
    own_in = lax.dynamic_slice_in_dim(inputs, group * B, B, 0).reshape(B, share, D)
    own_cot = lax.dynamic_slice_in_dim(cotangent, group * B, B, 0).reshape(B, share, D)

    def spread(x, users):
        x = x[None]
        for bit in range(1, bits):
            got = send(x, users, 1 << bit)
            high = (ti >> bit) % 2 == 1
            x = jnp.where(
                high, jnp.concatenate([got, x], 0), jnp.concatenate([x, got], 0)
            )
        return x.reshape(h, D)

    low_users = each([(0, 0, 0, 0), (0, 1, 0, 1)])
    high_users = each([(LAYERS - 1, 0, LAYERS - 1, 0), (LAYERS - 1, 1, LAYERS - 1, 1)])
    first_layer = layer == 0
    users = low_users + high_users
    seed = [
        spread(jnp.where(first_layer, own_in[b], own_cot[b]), users) for b in range(B)
    ]
    w = load_weights(weights[0])
    main = list(seed)
    rest = list(seed)
    saved = [[None] * LAYERS for _ in range(B)]
    slopes = [[None] * LAYERS for _ in range(B)]
    results = [jnp.zeros((share, D), bf16) for _ in range(B)]
    last = layer == LAYERS - 1

    for t in range(top + 1):
        forward = t < LAYERS
        backward = t >= LAYERS - 1
        mode = "mix" if forward and backward else ("fwd" if forward else "bwd")
        k, j = t, top - t
        swap, here, cross, along = [], [], [], []
        if forward:
            swap.append((k, 0, k, 1))
            here.append((k, 1, k, 1))
            if k + 1 < LAYERS:
                cross.append((k, 1, k + 1, 0))
                along.append((k, 1, k + 1, 1))
        if backward:
            swap.append((j, 1, j, 0))
            here.append((j, 0, j, 0))
            if j > 0:
                cross.append((j, 0, j - 1, 1))
                along.append((j, 0, j - 1, 0))
        joined = ([(k, 0, k, 0)] if forward else []) + ([(j, 1, j, 1)] if backward else [])
        swap, here, cross, along, joined = map(each, (swap, here, cross, along, joined))
        if t == LAYERS - 1:
            main = [jnp.where(last & ~up, seed[b], main[b]) for b in range(B)]
            rest = [jnp.where(last & up, seed[b], rest[b]) for b in range(B)]
        arrived = []
        for b in range(B):
            got = send(main[b], joined, 1)
            if forward:
                saved[b][k] = main[b]
                out, slopes[b][k] = first(mode, flag, main[b], got, gain, w)
            else:
                (out,) = first(mode, flag, main[b], got, gain, w)
            arrived.append(send(out, swap))
        fresh = []
        for b in range(B):
            keep, give = second(
                mode, flag, arrived[b], slopes[b][j] if backward else None, w
            )
            total = keep + send(give, here, 1).astype(f32)
            for bit in range(1, bits):
                mine = total.astype(bf16)
                got = send(mine, here, 1 << bit)
                if bit < bits - 1:
                    total = mine.astype(f32) + got.astype(f32)
            fresh.append(
                finish(mode, flag, mine, got, rest[b], saved[b][j] if backward else None, gain)
            )
        ok = jnp.zeros((), bool)
        if forward:
            ok = ok | (~up & (layer == k))
        if backward:
            ok = ok | (up & (layer == j))
        for b in range(B):
            mine = lax.dynamic_index_in_dim(
                fresh[b].reshape(hi, share, D), ti // 2, 0, keepdims=False
            )
            results[b] = jnp.where(ok, mine, results[b])
        if t < top:
            main = [send(fresh[b], cross) for b in range(B)]
            rest = [send(fresh[b], along) for b in range(B)]
            if t + 1 < LAYERS - 1:
                pass
    return jnp.stack(results).reshape(1, B, share * D)


def solution(mesh):
    placed = (P(None, "tensor"), P(None, "tensor"), P("section", None, "tensor"), P())
    return jax.shard_map(
        body, mesh=mesh, in_specs=placed, out_specs=P("section", None, "tensor"), check_vma=False
    )
```

```python
import functools

import jax
import jax.numpy as jnp
from jax import lax
from jax.experimental import pallas as pl
from jax.experimental.pallas import tpu as pltpu
from jax.sharding import PartitionSpec as P

LAYERS = 4
epsilon = 1e-05
AXES = ("section", "tensor")
f32, bf16 = jnp.float32, jnp.bfloat16
VMEM = pl.BlockSpec(memory_space=pltpu.VMEM)
SMEM = pl.BlockSpec(memory_space=pltpu.SMEM)
HBM = pl.BlockSpec(memory_space=pltpu.HBM)


def params(mib=4):
    return pltpu.CompilerParams(vmem_limit_bytes=mib * 1024 * 1024)


def tile_of(width):
    for tile in (512, 256, 128):
        if width % tile == 0:
            return tile
    return width


def gelu_both(v):
    c = 0.7978845608028654
    v2 = v * v
    th = jnp.tanh(c * v * (1.0 + 0.044715 * v2))
    half = 0.5 * (1.0 + th)
    slope = half + 0.5 * v * (1.0 - th * th) * (c * (1.0 + 3 * 0.044715 * v2))
    return v * half, slope


def inverse_rms_of(rows):
    return lax.rsqrt(jnp.mean(rows * rows, axis=-1, keepdims=True) + epsilon)


def load_weights(w, roles):
    def kernel(src, given, dst, kept, sem):
        copy = pltpu.make_async_copy(src, dst, sem)
        copy.start()
        for i in range(roles.shape[0]):
            kept[i] = given[i]
        copy.wait()

    return pl.pallas_call(
        kernel,
        in_specs=[HBM, SMEM],
        out_specs=[VMEM, SMEM],
        out_shape=[pltpu.VMEM(w.shape, w.dtype), pltpu.SMEM(roles.shape, roles.dtype)],
        scratch_shapes=[pltpu.SemaphoreType.DMA(())],
        compiler_params=params(2),
        name="load_weights",
    )(w, roles)


def first_kernel(mode, at, tile, flag, *refs):
    @pl.when(flag[at] != 0)
    def _():
        first_active(mode, at, tile, flag, *refs)


def first_active(mode, at, tile, flag, *refs):
    up = None
    if mode == "bwd":
        part, got, w, out, a = refs
    else:
        part, got, gain, w, out, slope, a = refs
        if mode == "mix":
            up = flag[at] == 1
    h = part.shape[0]
    for i, ref in enumerate((part, got)):
        if mode == "bwd":
            a[i * h:(i + 1) * h] = ref[...]
        else:
            x = ref[...].astype(f32)
            n = (x * inverse_rms_of(x) * gain[...]).astype(bf16)
            if up is not None:
                n = jnp.where(up, n, ref[...])
            a[i * h:(i + 1) * h] = n

    def step(i, carry):
        cols = pl.ds(pl.multiple_of(i * tile, tile), tile)
        y = jnp.dot(a[...], w[:, cols], preferred_element_type=f32)
        if mode == "bwd":
            out[:, cols] = y.astype(bf16)
        else:
            value, grad = gelu_both(y)
            slope[:, cols] = grad.astype(bf16)
            if up is not None:
                value = jnp.where(up, value, y)
            out[:, cols] = value.astype(bf16)
        return carry

    lax.fori_loop(0, w.shape[1] // tile, step, 0)


def first(mode, at, flag, part, got, gain, w):
    rows = 2 * part.shape[0]
    D, F = w.shape
    shape = jax.ShapeDtypeStruct((rows, F), bf16)
    args = (flag, part, got, w) if mode == "bwd" else (flag, part, got, gain, w)
    count = 1 if mode == "bwd" else 2
    return pl.pallas_call(
        functools.partial(first_kernel, mode, at, tile_of(F)),
        in_specs=[SMEM] + [VMEM] * (len(args) - 1),
        out_specs=[VMEM] * count,
        out_shape=[shape] * count,
        scratch_shapes=[pltpu.VMEM((rows, D), bf16)],
        compiler_params=params(),
        cost_estimate=pl.CostEstimate(
            flops=2 * rows * D * F, bytes_accessed=2 * D * F, transcendentals=rows * F
        ),
        name="first_" + mode,
    )(*args)


def second_kernel(mode, at, tile, flag, *refs):
    @pl.when(flag[at] != 0)
    def _():
        second_active(mode, at, tile, flag, *refs)


def second_active(mode, at, tile, flag, *refs):
    if mode == "fwd":
        arrived, w, keep, give, a = refs
    else:
        arrived, slope, w, keep, give, a = refs
    if mode == "fwd":
        a = arrived
    else:
        z = arrived[...]
        d = (z.astype(f32) * slope[...].astype(f32)).astype(bf16)
        if mode == "mix":
            d = jnp.where(flag[at] == 1, d, z)
        a[...] = d
    h = keep.shape[0]

    def step(i, carry):
        cols = pl.ds(pl.multiple_of(i * tile, tile), tile)
        y = lax.dot_general(
            a[...], w[cols, :], (((1,), (1,)), ((), ())), preferred_element_type=f32
        )
        keep[:, cols] = y[:h]
        give[:, cols] = y[h:].astype(bf16)
        return carry

    lax.fori_loop(0, w.shape[0] // tile, step, 0)


def second(mode, at, flag, arrived, slope, w):
    rows, F = arrived.shape
    D = w.shape[0]
    args = (flag, arrived, w) if mode == "fwd" else (flag, arrived, slope, w)
    return pl.pallas_call(
        functools.partial(second_kernel, mode, at, tile_of(D)),
        in_specs=[SMEM] + [VMEM] * (len(args) - 1),
        out_specs=[VMEM] * 2,
        out_shape=[
            jax.ShapeDtypeStruct((rows // 2, D), f32),
            jax.ShapeDtypeStruct((rows // 2, D), bf16),
        ],
        scratch_shapes=[pltpu.VMEM((rows, F), bf16)],
        compiler_params=params(),
        cost_estimate=pl.CostEstimate(
            flops=2 * rows * D * F, bytes_accessed=2 * D * F, transcendentals=0
        ),
        name="second_" + mode,
    )(*args)


def finish_kernel(mode, at, *refs):
    if mode == "fwd":
        total, got, rest, out = refs
        out[...] = (
            rest[...].astype(f32) + (total[...].astype(f32) + got[...].astype(f32))
        ).astype(bf16)
        return
    if mode == "bwd":
        total, got, rest, saved, gain, out = refs
    else:
        flag, total, got, rest, saved, gain, out = refs
    summed = total[...].astype(f32) + got[...].astype(f32)
    x = saved[...].astype(f32)
    scale = inverse_rms_of(x)
    unit = x * scale
    gu = summed * gain[...]
    delta = scale * (gu - unit * jnp.mean(gu * unit, axis=-1, keepdims=True))
    if mode == "mix":
        delta = jnp.where(flag[at] == 1, delta, summed)
    out[...] = (rest[...].astype(f32) + delta).astype(bf16)


def finish(mode, at, flag, total, got, rest, saved, gain):
    args = {
        "fwd": (total, got, rest),
        "bwd": (total, got, rest, saved, gain),
    }.get(mode, (flag, total, got, rest, saved, gain))
    specs = [VMEM] * len(args)
    if mode == "mix":
        specs[0] = SMEM
    return pl.pallas_call(
        functools.partial(finish_kernel, mode, at),
        in_specs=specs,
        out_specs=VMEM,
        out_shape=jax.ShapeDtypeStruct(rest.shape, bf16),
        compiler_params=params(),
        name="finish_" + mode,
    )(*args)


def body(inputs, cotangent, weights, norm_gains):
    S = lax.axis_size("section")
    T = lax.axis_size("tensor")
    stacks = S // (2 * LAYERS)
    stride = 2 * stacks
    si = lax.axis_index("section")
    ti = lax.axis_index("tensor")
    group = si % stride // 2
    layer = si // stride
    up = si % 2 == 0
    D = weights.shape[1]
    B = inputs.shape[0] // stacks
    share = inputs.shape[1] // D
    hi = T // 2
    h = hi * share
    top = 2 * (LAYERS - 1)
    bits = T.bit_length() - 1

    def send(x, pairs, flip=0):
        route = [(a * T + t, b * T + (t ^ flip)) for a, b in pairs for t in range(T)]
        return lax.ppermute(x, AXES, route)

    def section(k, q, down):
        return k * stride + 2 * q + down

    def each(pairs):
        return [(section(a, q, i), section(b, q, j)) for a, i, b, j in pairs for q in range(stacks)]

    steps = top + 1
    gain = lax.dynamic_index_in_dim(norm_gains, group * LAYERS + layer, 0, keepdims=True)
    own_in = lax.dynamic_slice_in_dim(inputs, group * B, B, 0)
    own_cot = lax.dynamic_slice_in_dim(cotangent, group * B, B, 0)
    own = jnp.where(layer == 0, own_in, own_cot).reshape(B, share, D)
    tick = jnp.arange(steps, dtype=jnp.int32)
    ahead = tick == layer
    behind = tick == top - layer
    roles = jnp.concatenate([
        jnp.where(up, jnp.where(ahead, 1, 0), jnp.where(behind, 2, 0)),
        jnp.where(up, jnp.where(behind, 1, 0), jnp.where(ahead, 2, 0)),
    ]).astype(jnp.int32)
    oks = [jnp.where(up, top - layer, layer) == t for t in range(steps)]
    last = layer == LAYERS - 1
    seed_main, seed_rest = last & ~up, last & up
    high = ti // 2
    highs = [(ti >> bit) % 2 == 1 for bit in range(1, bits)]
    w, own, gain, roles, oks, seed_main, seed_rest, high, highs = lax.optimization_barrier(
        (weights[0], own, gain, roles, oks, seed_main, seed_rest, high, highs)
    )

    def spread(x, users):
        x = x[None]
        for bit in range(1, bits):
            got = send(x, users, 1 << bit)
            got, _ = lax.optimization_barrier((got, roles))
            x = jnp.where(
                highs[bit - 1], jnp.concatenate([got, x], 0), jnp.concatenate([x, got], 0)
            )
        return x.reshape(h, D)

    everyone = [(s, s) for s in range(S)]
    w, roles = load_weights(w, roles)
    seed = []
    for b in range(B):
        seed.append(spread(own[b], everyone))
    main = list(seed)
    rest = list(seed)
    saved = [[None] * LAYERS for _ in range(B)]
    slopes = [[None] * LAYERS for _ in range(B)]
    results = [jnp.zeros((share, D), bf16) for _ in range(B)]

    for t in range(top + 1):
        forward = t < LAYERS
        backward = t >= LAYERS - 1
        mode = "mix" if forward and backward else ("fwd" if forward else "bwd")
        k, j = t, top - t
        swap, cross, along = [], [], []
        if forward:
            swap.append((k, 0, k, 1))
            if k + 1 < LAYERS:
                cross.append((k, 1, k + 1, 0))
                along.append((k, 1, k + 1, 1))
        if backward:
            swap.append((j, 1, j, 0))
            if j > 0:
                cross.append((j, 0, j - 1, 1))
                along.append((j, 0, j - 1, 0))
        swap, cross, along = each(swap), each(cross), each(along)
        if t == LAYERS - 1:
            main = [jnp.where(seed_main, seed[b], main[b]) for b in range(B)]
            rest = [jnp.where(seed_rest, seed[b], rest[b]) for b in range(B)]
        arrived = []
        for b in range(B):
            got = send(main[b], everyone, 1)
            if forward:
                saved[b][k] = main[b]
                out, slopes[b][k] = first(mode, t, roles, main[b], got, gain, w)
            else:
                (out,) = first(mode, t, roles, main[b], got, gain, w)
            arrived.append(send(out, swap))
        fresh = []
        for b in range(B):
            _, _, arrived[b] = lax.optimization_barrier((rest[b], fresh[-1:], arrived[b]))
            keep, give = second(
                mode, steps + t, roles, arrived[b], slopes[b][j] if backward else None, w
            )
            total = keep + send(give, everyone, 1).astype(f32)
            for bit in range(1, bits):
                mine = total.astype(bf16)
                got = send(mine, everyone, 1 << bit)
                if bit < bits - 1:
                    total = mine.astype(f32) + got.astype(f32)
            fresh.append(
                finish(mode, steps + t, roles, mine, got, rest[b], saved[b][j] if backward else None, gain)
            )
        for b in range(B):
            mine = lax.dynamic_index_in_dim(
                fresh[b].reshape(hi, share, D), high, 0, keepdims=False
            )
            results[b] = jnp.where(oks[t], mine, results[b])
        if t < top:
            main = [send(fresh[b], cross) for b in range(B)]
            rest = [send(fresh[b], along) for b in range(B)]
    return jnp.stack(results).reshape(1, B, share * D)


def solution(mesh):
    placed = (P(None, "tensor"), P(None, "tensor"), P("section", None, "tensor"), P())
    return jax.shard_map(
        body, mesh=mesh, in_specs=placed, out_specs=P("section", None, "tensor"), check_vma=False
    )
```

```python
import functools

import jax
import jax.numpy as jnp
from jax import lax
from jax.experimental import pallas as pl
from jax.experimental.pallas import tpu as pltpu
from jax.sharding import PartitionSpec as P


LAYERS = 4
epsilon = 1e-05
AXES = ("section", "tensor")
f32, bf16 = jnp.float32, jnp.bfloat16
VMEM = pl.BlockSpec(memory_space=pltpu.VMEM)
SMEM = pl.BlockSpec(memory_space=pltpu.SMEM)
HBM = pl.BlockSpec(memory_space=pltpu.HBM)


def params(mib=4):
    return pltpu.CompilerParams(vmem_limit_bytes=mib * 1024 * 1024)


def tile_of(width):
    for tile in (512, 256, 128):
        if width % tile == 0:
            return tile
    return width


def gelu_both(v):
    c = 0.7978845608028654
    v2 = v * v
    th = jnp.tanh(c * v * (1.0 + 0.044715 * v2))
    half = 0.5 * (1.0 + th)
    slope = half + 0.5 * v * (1.0 - th * th) * (c * (1.0 + 3 * 0.044715 * v2))
    return v * half, slope


def inverse_rms_of(rows):
    return lax.rsqrt(jnp.mean(rows * rows, axis=-1, keepdims=True) + epsilon)


def load_weights(w, roles):
    def kernel(src, given, dst, kept, sem):
        copy = pltpu.make_async_copy(src, dst, sem)
        copy.start()
        for i in range(roles.shape[0]):
            kept[i] = given[i]
        copy.wait()

    return pl.pallas_call(
        kernel,
        in_specs=[HBM, SMEM],
        out_specs=[VMEM, SMEM],
        out_shape=[pltpu.VMEM(w.shape, w.dtype), pltpu.SMEM(roles.shape, roles.dtype)],
        scratch_shapes=[pltpu.SemaphoreType.DMA(())],
        compiler_params=params(2),
        name="load_weights",
    )(w, roles)


def first_kernel(mode, at, tile, flag, *refs):
    @pl.when(flag[at] != 0)
    def _():
        first_active(mode, at, tile, flag, *refs)


def first_active(mode, at, tile, flag, *refs):
    up = None
    if mode == "bwd":
        part, got, w, out, a = refs
    else:
        part, got, gain, w, out, slope, a = refs
        if mode == "mix":
            up = flag[at] == 1
    h = part.shape[0]
    for i, ref in enumerate((part, got)):
        if mode == "bwd":
            a[i * h:(i + 1) * h] = ref[...]
        else:
            x = ref[...].astype(f32)
            n = (x * inverse_rms_of(x) * gain[...]).astype(bf16)
            if up is not None:
                n = jnp.where(up, n, ref[...])
            a[i * h:(i + 1) * h] = n

    def step(i, carry):
        cols = pl.ds(pl.multiple_of(i * tile, tile), tile)
        y = jnp.dot(a[...], w[:, cols], preferred_element_type=f32)
        if mode == "bwd":
            out[:, cols] = y.astype(bf16)
        else:
            value, grad = gelu_both(y)
            slope[:, cols] = grad.astype(bf16)
            if up is not None:
                value = jnp.where(up, value, y)
            out[:, cols] = value.astype(bf16)
        return carry

    lax.fori_loop(0, w.shape[1] // tile, step, 0)


def first(mode, at, flag, part, got, gain, w):
    rows = 2 * part.shape[0]
    D, F = w.shape
    shape = jax.ShapeDtypeStruct((rows, F), bf16)
    args = (flag, part, got, w) if mode == "bwd" else (flag, part, got, gain, w)
    count = 1 if mode == "bwd" else 2
    return pl.pallas_call(
        functools.partial(first_kernel, mode, at, tile_of(F)),
        in_specs=[SMEM] + [VMEM] * (len(args) - 1),
        out_specs=[VMEM] * count,
        out_shape=[shape] * count,
        scratch_shapes=[pltpu.VMEM((rows, D), bf16)],
        compiler_params=params(),
        cost_estimate=pl.CostEstimate(
            flops=2 * rows * D * F, bytes_accessed=2 * D * F, transcendentals=rows * F
        ),
    )(*args)


def second_kernel(mode, at, tile, flag, *refs):
    @pl.when(flag[at] != 0)
    def _():
        second_active(mode, at, tile, flag, *refs)


def second_active(mode, at, tile, flag, *refs):
    if mode == "fwd":
        arrived, w, keep, give, a = refs
    else:
        arrived, slope, w, keep, give, a = refs
    if mode == "fwd":
        a = arrived
    else:
        z = arrived[...]
        d = (z.astype(f32) * slope[...].astype(f32)).astype(bf16)
        if mode == "mix":
            d = jnp.where(flag[at] == 1, d, z)
        a[...] = d
    h = keep.shape[0]

    def step(i, carry):
        cols = pl.ds(pl.multiple_of(i * tile, tile), tile)
        y = lax.dot_general(
            a[...], w[cols, :], (((1,), (1,)), ((), ())), preferred_element_type=f32
        )
        keep[:, cols] = y[:h]
        give[:, cols] = y[h:].astype(bf16)
        return carry

    lax.fori_loop(0, w.shape[0] // tile, step, 0)


def second(mode, at, flag, arrived, slope, w):
    rows, F = arrived.shape
    D = w.shape[0]
    args = (flag, arrived, w) if mode == "fwd" else (flag, arrived, slope, w)
    return pl.pallas_call(
        functools.partial(second_kernel, mode, at, tile_of(D)),
        in_specs=[SMEM] + [VMEM] * (len(args) - 1),
        out_specs=[VMEM] * 2,
        out_shape=[
            jax.ShapeDtypeStruct((rows // 2, D), f32),
            jax.ShapeDtypeStruct((rows // 2, D), bf16),
        ],
        scratch_shapes=[pltpu.VMEM((rows, F), bf16)],
        compiler_params=params(),
        cost_estimate=pl.CostEstimate(
            flops=2 * rows * D * F, bytes_accessed=2 * D * F, transcendentals=0
        ),
    )(*args)


def finish_kernel(mode, at, *refs):
    if mode == "fwd":
        total, got, rest, out = refs
        out[...] = (
            rest[...].astype(f32) + (total[...].astype(f32) + got[...].astype(f32))
        ).astype(bf16)
        return
    if mode == "bwd":
        total, got, rest, saved, gain, out = refs
    else:
        flag, total, got, rest, saved, gain, out = refs
    summed = total[...].astype(f32) + got[...].astype(f32)
    x = saved[...].astype(f32)
    scale = inverse_rms_of(x)
    unit = x * scale
    gu = summed * gain[...]
    delta = scale * (gu - unit * jnp.mean(gu * unit, axis=-1, keepdims=True))
    if mode == "mix":
        delta = jnp.where(flag[at] == 1, delta, summed)
    out[...] = (rest[...].astype(f32) + delta).astype(bf16)


def finish(mode, at, flag, total, got, rest, saved, gain):
    args = {
        "fwd": (total, got, rest),
        "bwd": (total, got, rest, saved, gain),
    }.get(mode, (flag, total, got, rest, saved, gain))
    specs = [VMEM] * len(args)
    if mode == "mix":
        specs[0] = SMEM
    return pl.pallas_call(
        functools.partial(finish_kernel, mode, at),
        in_specs=specs,
        out_specs=VMEM,
        out_shape=jax.ShapeDtypeStruct(rest.shape, bf16),
        compiler_params=params(),
    )(*args)


def body(inputs, cotangent, weights, norm_gains):
    S = lax.axis_size("section")
    T = lax.axis_size("tensor")
    stacks = S // (2 * LAYERS)
    stride = 2 * stacks
    si = lax.axis_index("section")
    ti = lax.axis_index("tensor")
    group = si % stride // 2
    layer = si // stride
    up = si % 2 == 0
    D = weights.shape[1]
    B = inputs.shape[0] // stacks
    share = inputs.shape[1] // D
    hi = T // 2
    h = hi * share
    top = 2 * (LAYERS - 1)
    bits = T.bit_length() - 1

    def send(x, pairs, flip=0):
        route = [(a * T + t, b * T + (t ^ flip)) for a, b in pairs for t in range(T)]
        return lax.ppermute(x, AXES, route)

    def section(k, q, down):
        return k * stride + 2 * q + down

    def each(pairs):
        return [(section(a, q, i), section(b, q, j)) for a, i, b, j in pairs for q in range(stacks)]

    steps = top + 1
    gain = lax.dynamic_index_in_dim(norm_gains, group * LAYERS + layer, 0, keepdims=True)
    own_in = lax.dynamic_slice_in_dim(inputs, group * B, B, 0)
    own_cot = lax.dynamic_slice_in_dim(cotangent, group * B, B, 0)
    own = jnp.where(layer == 0, own_in, own_cot).reshape(B, share, D)
    tick = jnp.arange(steps, dtype=jnp.int32)
    ahead = tick == layer
    behind = tick == top - layer
    roles = jnp.concatenate([
        jnp.where(up, jnp.where(ahead, 1, 0), jnp.where(behind, 2, 0)),
        jnp.where(up, jnp.where(behind, 1, 0), jnp.where(ahead, 2, 0)),
    ]).astype(jnp.int32)
    oks = [jnp.where(up, top - layer, layer) == t for t in range(steps)]
    last = layer == LAYERS - 1
    seed_main, seed_rest = last & ~up, last & up
    high = ti // 2
    highs = [(ti >> bit) % 2 == 1 for bit in range(1, bits)]
    w, own, gain, roles, oks, seed_main, seed_rest, high, highs = lax.optimization_barrier(
        (weights[0], own, gain, roles, oks, seed_main, seed_rest, high, highs)
    )

    def spread(x, users, gate):
        x = x[None]
        for bit in range(1, bits):
            got = send(x, users, 1 << bit)
            got, _ = lax.optimization_barrier((got, gate))
            x = jnp.where(
                highs[bit - 1], jnp.concatenate([got, x], 0), jnp.concatenate([x, got], 0)
            )
        return x.reshape(h, D)

    everyone = [(s, s) for s in range(S)]
    w, roles = load_weights(w, roles)
    seed = [spread(own[0], everyone, roles)] + [None] * (B - 1)
    main = list(seed)
    rest = list(seed)
    saved = [[None] * LAYERS for _ in range(B)]
    slopes = [[None] * LAYERS for _ in range(B)]
    results = [jnp.zeros((share, D), bf16) for _ in range(B)]

    def plan(t):
        forward = t < LAYERS
        backward = t >= LAYERS - 1
        mode = "mix" if forward and backward else ("fwd" if forward else "bwd")
        k, j = t, top - t
        swap, cross, along = [], [], []
        if forward:
            swap.append((k, 0, k, 1))
            if k + 1 < LAYERS:
                cross.append((k, 1, k + 1, 0))
                along.append((k, 1, k + 1, 1))
        if backward:
            swap.append((j, 1, j, 0))
            if j > 0:
                cross.append((j, 0, j - 1, 1))
                along.append((j, 0, j - 1, 0))
        return forward, backward, mode, k, j, each(swap), each(cross), each(along)

    def phase_one(t, b):
        forward, _, mode, k, _, _, _, _ = plan(t)
        if t == 0 and b > 0:
            seed[b] = main[b] = rest[b] = spread(own[b], everyone, outs[0])
        if t == LAYERS - 1:
            main[b] = jnp.where(seed_main, seed[b], main[b])
        got = send(main[b], everyone, 1)
        if forward:
            saved[b][k] = main[b]
            outs[b], slopes[b][k] = first(mode, t, roles, main[b], got, gain, w)
        else:
            (outs[b],) = first(mode, t, roles, main[b], got, gain, w)
        if t == LAYERS - 1:
            late, _ = lax.optimization_barrier((rest[b], outs[b]))
            rest[b] = jnp.where(seed_rest, seed[b], late)

    outs = [None] * B
    phase_one(0, 0)
    for t in range(top + 1):
        _, backward, mode, _, j, swap, cross, along = plan(t)
        arrived = send(outs[0], swap, 0)
        gate = outs[0]
        for b in range(B):
            if b + 1 < B:
                phase_one(t, b + 1)
            arrived = lax.optimization_barrier((arrived, rest[b], gate))[0]
            keep, give = second(
                mode, steps + t, roles, arrived, slopes[b][j] if backward else None, w
            )
            if b + 1 < B:
                arrived = send(outs[b + 1], swap, 0)
            total = keep + send(give, everyone, 1).astype(f32)
            for bit in range(1, bits):
                mine = total.astype(bf16)
                got = send(mine, everyone, 1 << bit)
                if bit < bits - 1:
                    total = mine.astype(f32) + got.astype(f32)
            fresh = finish(
                mode, steps + t, roles, mine, got, rest[b],
                saved[b][j] if backward else None, gain,
            )
            gate = fresh
            piece = lax.dynamic_index_in_dim(
                fresh.reshape(hi, share, D), high, 0, keepdims=False
            )
            results[b] = jnp.where(oks[t], piece, results[b])
            if t < top:
                if b > 0:
                    fresh = lax.optimization_barrier((fresh, outs[0]))[0]
                main[b] = send(fresh, cross, 0)
                rest[b] = send(fresh, along, 0)
                if b == 0:
                    phase_one(t + 1, 0)
    return jnp.stack(results).reshape(1, B, share * D)


def solution(mesh):
    placed = (P(None, "tensor"), P(None, "tensor"), P("section", None, "tensor"), P())
    return jax.shard_map(
        body, mesh=mesh, in_specs=placed, out_specs=P("section", None, "tensor"), check_vma=False
    )
```

```python
import functools

import jax
import jax.numpy as jnp
from jax import lax
from jax.experimental import pallas as pl
from jax.experimental.pallas import tpu as pltpu
from jax.sharding import PartitionSpec as P


LAYERS = 4
epsilon = 1e-05
AXES = ("section", "tensor")
f32, bf16 = jnp.float32, jnp.bfloat16
VMEM = pl.BlockSpec(memory_space=pltpu.VMEM)
SMEM = pl.BlockSpec(memory_space=pltpu.SMEM)
HBM = pl.BlockSpec(memory_space=pltpu.HBM)


def params(mib=4):
    return pltpu.CompilerParams(vmem_limit_bytes=mib * 1024 * 1024)


def tile_of(width):
    for tile in (512, 256, 128):
        if width % tile == 0:
            return tile
    return width


def gelu_both(v):
    c = 0.7978845608028654
    v2 = v * v
    th = jnp.tanh(c * v * (1.0 + 0.044715 * v2))
    half = 0.5 * (1.0 + th)
    slope = half + 0.5 * v * (1.0 - th * th) * (c * (1.0 + 3 * 0.044715 * v2))
    return v * half, slope


def inverse_rms_of(rows):
    return lax.rsqrt(jnp.mean(rows * rows, axis=-1, keepdims=True) + epsilon)


def load_weights(w, roles):
    def kernel(src, given, dst, kept, sem):
        copy = pltpu.make_async_copy(src, dst, sem)
        copy.start()
        for i in range(roles.shape[0]):
            kept[i] = given[i]
        copy.wait()

    return pl.pallas_call(
        kernel,
        in_specs=[HBM, SMEM],
        out_specs=[VMEM, SMEM],
        out_shape=[pltpu.VMEM(w.shape, w.dtype), pltpu.SMEM(roles.shape, roles.dtype)],
        scratch_shapes=[pltpu.SemaphoreType.DMA(())],
        compiler_params=params(2),
        name="load_weights",
    )(w, roles)


def first_kernel(mode, at, tile, flag, *refs):
    @pl.when(flag[at] != 0)
    def _():
        first_active(mode, at, tile, flag, *refs)


def first_active(mode, at, tile, flag, *refs):
    up = None
    if mode == "bwd":
        part, got, w, out, a = refs
    else:
        part, got, gain, w, out, slope, a = refs
        if mode == "mix":
            up = flag[at] == 1
    h = part.shape[0]
    for i, ref in enumerate((part, got)):
        if mode == "bwd":
            a[i * h:(i + 1) * h] = ref[...]
        else:
            x = ref[...].astype(f32)
            n = (x * inverse_rms_of(x) * gain[...]).astype(bf16)
            if up is not None:
                n = jnp.where(up, n, ref[...])
            a[i * h:(i + 1) * h] = n

    def step(i, carry):
        cols = pl.ds(pl.multiple_of(i * tile, tile), tile)
        y = jnp.dot(a[...], w[:, cols], preferred_element_type=f32)
        if mode == "bwd":
            out[:, cols] = y.astype(bf16)
        else:
            value, grad = gelu_both(y)
            slope[:, cols] = grad.astype(bf16)
            if up is not None:
                value = jnp.where(up, value, y)
            out[:, cols] = value.astype(bf16)
        return carry

    lax.fori_loop(0, w.shape[1] // tile, step, 0)


def first(mode, at, flag, part, got, gain, w):
    rows = 2 * part.shape[0]
    D, F = w.shape
    shape = jax.ShapeDtypeStruct((rows, F), bf16)
    args = (flag, part, got, w) if mode == "bwd" else (flag, part, got, gain, w)
    count = 1 if mode == "bwd" else 2
    return pl.pallas_call(
        functools.partial(first_kernel, mode, at, tile_of(F)),
        in_specs=[SMEM] + [VMEM] * (len(args) - 1),
        out_specs=[VMEM] * count,
        out_shape=[shape] * count,
        scratch_shapes=[pltpu.VMEM((rows, D), bf16)],
        compiler_params=params(),
        cost_estimate=pl.CostEstimate(
            flops=2 * rows * D * F, bytes_accessed=2 * D * F, transcendentals=rows * F
        ),
    )(*args)


def second_kernel(mode, at, tile, flag, *refs):
    @pl.when(flag[at] != 0)
    def _():
        second_active(mode, at, tile, flag, *refs)


def second_active(mode, at, tile, flag, *refs):
    if mode == "fwd":
        arrived, w, keep, give, a = refs
    else:
        arrived, slope, w, keep, give, a = refs
    if mode == "fwd":
        a = arrived
    else:
        z = arrived[...]
        d = (z.astype(f32) * slope[...].astype(f32)).astype(bf16)
        if mode == "mix":
            d = jnp.where(flag[at] == 1, d, z)
        a[...] = d
    h = keep.shape[0]

    def step(i, carry):
        cols = pl.ds(pl.multiple_of(i * tile, tile), tile)
        y = lax.dot_general(
            a[...], w[cols, :], (((1,), (1,)), ((), ())), preferred_element_type=f32
        )
        keep[:, cols] = y[:h]
        give[:, cols] = y[h:].astype(bf16)
        return carry

    lax.fori_loop(0, w.shape[0] // tile, step, 0)


def second(mode, at, flag, arrived, slope, w):
    rows, F = arrived.shape
    D = w.shape[0]
    args = (flag, arrived, w) if mode == "fwd" else (flag, arrived, slope, w)
    return pl.pallas_call(
        functools.partial(second_kernel, mode, at, D // 2 if D % 256 == 0 else tile_of(D)),
        in_specs=[SMEM] + [VMEM] * (len(args) - 1),
        out_specs=[VMEM] * 2,
        out_shape=[
            jax.ShapeDtypeStruct((rows // 2, D), f32),
            jax.ShapeDtypeStruct((rows // 2, D), bf16),
        ],
        scratch_shapes=[pltpu.VMEM((rows, F), bf16)],
        compiler_params=params(),
        cost_estimate=pl.CostEstimate(
            flops=2 * rows * D * F, bytes_accessed=2 * D * F, transcendentals=0
        ),
    )(*args)


def finish_kernel(mode, at, *refs):
    if mode == "fwd":
        total, got, rest, out = refs
        out[...] = (
            rest[...].astype(f32) + (total[...].astype(f32) + got[...].astype(f32))
        ).astype(bf16)
        return
    if mode == "bwd":
        total, got, rest, saved, gain, out = refs
    else:
        flag, total, got, rest, saved, gain, out = refs
    summed = total[...].astype(f32) + got[...].astype(f32)
    x = saved[...].astype(f32)
    scale = inverse_rms_of(x)
    unit = x * scale
    gu = summed * gain[...]
    delta = scale * (gu - unit * jnp.mean(gu * unit, axis=-1, keepdims=True))
    if mode == "mix":
        delta = jnp.where(flag[at] == 1, delta, summed)
    out[...] = (rest[...].astype(f32) + delta).astype(bf16)


def finish(mode, at, flag, total, got, rest, saved, gain):
    args = {
        "fwd": (total, got, rest),
        "bwd": (total, got, rest, saved, gain),
    }.get(mode, (flag, total, got, rest, saved, gain))
    specs = [VMEM] * len(args)
    if mode == "mix":
        specs[0] = SMEM
    return pl.pallas_call(
        functools.partial(finish_kernel, mode, at),
        in_specs=specs,
        out_specs=VMEM,
        out_shape=jax.ShapeDtypeStruct(rest.shape, bf16),
        compiler_params=params(),
    )(*args)


def body(inputs, cotangent, weights, norm_gains):
    S = lax.axis_size("section")
    T = lax.axis_size("tensor")
    stacks = S // (2 * LAYERS)
    stride = 2 * stacks
    si = lax.axis_index("section")
    ti = lax.axis_index("tensor")
    group = si % stride // 2
    layer = si // stride
    up = si % 2 == 0
    D = weights.shape[1]
    B = inputs.shape[0] // stacks
    share = inputs.shape[1] // D
    hi = T // 2
    h = hi * share
    top = 2 * (LAYERS - 1)
    bits = T.bit_length() - 1

    def send(x, pairs, flip=0):
        route = [(a * T + t, b * T + (t ^ flip)) for a, b in pairs for t in range(T)]
        return lax.ppermute(x, AXES, route)

    def section(k, q, down):
        return k * stride + 2 * q + down

    def each(pairs):
        return [(section(a, q, i), section(b, q, j)) for a, i, b, j in pairs for q in range(stacks)]

    steps = top + 1
    gain = lax.dynamic_index_in_dim(norm_gains, group * LAYERS + layer, 0, keepdims=True)
    own_in = lax.dynamic_slice_in_dim(inputs, group * B, B, 0)
    own_cot = lax.dynamic_slice_in_dim(cotangent, group * B, B, 0)
    own = jnp.where(layer == 0, own_in, own_cot).reshape(B, share, D)
    tick = jnp.arange(steps, dtype=jnp.int32)
    ahead = tick == layer
    behind = tick == top - layer
    roles = jnp.concatenate([
        jnp.where(up, jnp.where(ahead, 1, 0), jnp.where(behind, 2, 0)),
        jnp.where(up, jnp.where(behind, 1, 0), jnp.where(ahead, 2, 0)),
    ]).astype(jnp.int32)
    oks = [jnp.where(up, top - layer, layer) == t for t in range(steps)]
    last = layer == LAYERS - 1
    seed_main, seed_rest = last & ~up, last & up
    high = ti // 2
    highs = [(ti >> bit) % 2 == 1 for bit in range(1, bits)]
    w, own, gain, roles, oks, seed_main, seed_rest, high, highs = lax.optimization_barrier(
        (weights[0], own, gain, roles, oks, seed_main, seed_rest, high, highs)
    )

    def spread(x, users, gate):
        x = x[None]
        for bit in range(1, bits):
            got = send(x, users, 1 << bit)
            got, _ = lax.optimization_barrier((got, gate))
            x = jnp.where(
                highs[bit - 1], jnp.concatenate([got, x], 0), jnp.concatenate([x, got], 0)
            )
        return x.reshape(h, D)

    everyone = [(s, s) for s in range(S)]
    w, roles = load_weights(pltpu.with_memory_space_constraint(w, pltpu.HBM), roles)
    seed = [spread(own[0], everyone, roles)] + [None] * (B - 1)
    main = list(seed)
    rest = list(seed)
    saved = [[None] * LAYERS for _ in range(B)]
    slopes = [[None] * LAYERS for _ in range(B)]
    results = [jnp.zeros((share, D), bf16) for _ in range(B)]

    def plan(t):
        forward = t < LAYERS
        backward = t >= LAYERS - 1
        mode = "mix" if forward and backward else ("fwd" if forward else "bwd")
        k, j = t, top - t
        swap, cross, along = [], [], []
        if forward:
            swap.append((k, 0, k, 1))
            if k + 1 < LAYERS:
                cross.append((k, 1, k + 1, 0))
                along.append((k, 1, k + 1, 1))
        if backward:
            swap.append((j, 1, j, 0))
            if j > 0:
                cross.append((j, 0, j - 1, 1))
                along.append((j, 0, j - 1, 0))
        return forward, backward, mode, k, j, each(swap), each(cross), each(along)

    def phase_one(t, b):
        forward, _, mode, k, _, _, _, _ = plan(t)
        if t == 0 and b > 0:
            seed[b] = main[b] = rest[b] = spread(own[b], everyone, outs[0])
        if t == LAYERS - 1:
            main[b] = jnp.where(seed_main, seed[b], main[b])
        got = send(main[b], everyone, 1)
        if forward:
            saved[b][k] = main[b]
            outs[b], slopes[b][k] = first(mode, t, roles, main[b], got, gain, w)
        else:
            (outs[b],) = first(mode, t, roles, main[b], got, gain, w)
        if t == LAYERS - 1:
            late, _ = lax.optimization_barrier((rest[b], outs[b]))
            rest[b] = jnp.where(seed_rest, seed[b], late)

    outs = [None] * B
    phase_one(0, 0)
    for t in range(top + 1):
        _, backward, mode, _, j, swap, cross, along = plan(t)
        arrived = send(outs[0], swap, 0)
        gate = outs[0]
        for b in range(B):
            if b + 1 < B:
                phase_one(t, b + 1)
            arrived = lax.optimization_barrier((arrived, rest[b], gate))[0]
            keep, give = second(
                mode, steps + t, roles, arrived, slopes[b][j] if backward else None, w
            )
            if b + 1 < B:
                arrived = send(outs[b + 1], swap, 0)
            total = keep + send(give, everyone, 1).astype(f32)
            for bit in range(1, bits):
                mine = total.astype(bf16)
                got = send(mine, everyone, 1 << bit)
                if bit < bits - 1:
                    total = mine.astype(f32) + got.astype(f32)
            fresh = finish(
                mode, steps + t, roles, mine, got, rest[b],
                saved[b][j] if backward else None, gain,
            )
            gate = fresh
            piece = lax.dynamic_index_in_dim(fresh.reshape(hi, share, D), high, 0, keepdims=False)
            results[b] = jnp.where(oks[t], piece, results[b])
            if t < top:
                if b > 0:
                    fresh = lax.optimization_barrier((fresh, outs[0]))[0]
                main[b] = send(fresh, cross, 0)
                rest[b] = send(fresh, along, 0)
                if b == 0:
                    phase_one(t + 1, 0)
    return jnp.stack(results).reshape(1, B, share * D)


def solution(mesh):
    placed = (P(None, "tensor"), P(None, "tensor"), P("section", None, "tensor"), P())
    return jax.shard_map(
        body, mesh=mesh, in_specs=placed, out_specs=P("section", None, "tensor"), check_vma=False
    )
```
